256 devices in a mesh: owner: 8 (over x, core), rows: 32 (over z, y).
Axes of the slice: x: 4, y: 4, z: 8, core: 2. Of those that a mesh axis runs over, the one named last changes fastest.
Arguments:
- w_down: float32 [16, 6400, 4096], P('owner', None, 'rows'), may hold values from -0.15625 to 0.15625
- avg_down: bfloat16 [16, 6400, 4096], P('owner', None, 'rows'), may hold values from -0.0390625 to 0.0390625
- router_weight: float32 [4096, 16], P('rows', 'owner'), may hold values from -0.09375 to 0.09375
- router_gain: float32 [4096], P('rows'), may hold values from 0.25 to 1.75
Outputs:
- serve_down: bfloat16 [16, 6400, 4096], P('owner', 'rows')
- scale_down: float32 [16, 6400], P('owner', 'rows')
- serve_router: bfloat16 [4096, 16], replicated
The draws below stay inside these ranges and needn't reach their ends.
All inputs are finite; a program needn't handle non-finite values. Where the reference program divides by a largest or mean magnitude, that divisor is 1e-20 or more.
Results may differ from the reference program's by a relative error of at most 0.001.
Values may be sent and summed in bfloat16 or wider, within the bound.
A program may use at most 64 MiB of HBM per device.

```python
import jax
import jax.numpy as jnp

EXPERTS = 16
D_MODEL = 4096
D_EXPERT = 6400


def strengthened(values, stream_key, source, target, parts, factor):
    def block_of(position):
        return (jnp.arange(values.shape[position]) // (values.shape[position] // parts)).reshape((-1,) + (1,) * (values.ndim - 1 - position))

    one_side = jax.random.permutation(stream_key, parts)[block_of(target)]
    second = (block_of(target) + parts // 2) % parts
    return jnp.where((block_of(source) == one_side) | (block_of(source) == second), factor * values, values)


def shard_levels(rng, dims, cuts, least, high):
    loudness = 1.0
    for dim, parts in cuts:
        draws = jax.random.uniform(jax.random.fold_in(jax.random.fold_in(rng, 6), dim), (parts,), jnp.float32, least / len(cuts), high / len(cuts))
        loudness = loudness * jnp.repeat(jnp.exp(draws), dims[dim] // parts).reshape((-1,) + (1,) * (len(dims) - 1 - dim))
    return loudness


def centred(key, extent, deviation, reach, shards=(), held_as=jnp.bfloat16):
    level = shard_levels(key, extent, shards, -0.22, 0.18) if shards else 1.0
    array = jax.random.normal(key, extent, jnp.float32) * deviation * level
    return jnp.minimum(jnp.maximum(array, -reach), reach).astype(held_as)


def bell_draw_with(stream_key, dims, width, limit, shards, heavy, dtype=jnp.bfloat16):
    result = width * jax.random.normal(stream_key, dims, jnp.float32)
    if shards:
        result = result * shard_levels(stream_key, dims, shards, -0.22, 0.18)
    return jnp.clip(strengthened(result, jax.random.fold_in(stream_key, 3), *heavy), -limit, limit).astype(dtype)


def setup_inputs(seed: int = 0) -> dict:
    seeds = jax.random.split(jax.random.key(seed), 5)
    w_down = bell_draw_with(seeds[0], (EXPERTS, D_EXPERT, D_MODEL), D_EXPERT ** -0.5, 0.15625, ((0, 8), (2, 32)), (2, 1, 32, 2.75), jnp.float32)
    avg_down = centred(seeds[1], (EXPERTS, D_EXPERT, D_MODEL), (D_EXPERT * 4) ** -0.5, 0.0390625, ((0, 8), (2, 32)))
    router_weight = centred(seeds[2], (D_MODEL, EXPERTS), D_MODEL ** -0.5, 0.09375, ((0, 32), (1, 8)), jnp.float32)
    router_gain = jnp.clip(1.0 + 0.15 * jax.random.normal(seeds[3], (D_MODEL,), jnp.float32), 0.25, 1.75)
    return dict(w_down=w_down, avg_down=avg_down, router_weight=router_weight, router_gain=router_gain)


def reference(w_down, avg_down, router_weight, router_gain):
    fresh_down = w_down + avg_down.astype(jnp.float32)
    scale_down = jnp.sum(jnp.abs(fresh_down), axis=2) / D_MODEL
    serve_down = (fresh_down / jnp.expand_dims(scale_down, 2)).astype(jnp.bfloat16)
    serve_router = (router_weight * router_gain[:, None]).astype(jnp.bfloat16)
    return serve_down, scale_down, serve_router
```

```python
import functools

import jax
import jax.numpy as jnp
from jax import lax
from jax.experimental import pallas as pl
from jax.experimental.pallas import tpu as pltpu
from jax.sharding import PartitionSpec as P

MESH = pl.DeviceIdType.MESH
LANES = 128
HEAD = 8
SPLIT = 96


def exchange(
    n_rows, n_owner, ny, d_model,
    w_ref, a_ref, rw_ref, rg_ref,
    out_ref, scale_ref, rall_ref,
    rwbuf, rgbuf, wbuf, abuf, stage, heads_out, heads_in, sums_out, sums_in, scales, mine, rpart, rrow,
    rw_sem, rg_sem, w_sem, a_sem, rs_send, rs_recv, ag_send, ag_recv, head_send, head_recv,
    bulk_send, bulk_recv, r1_send, r1_recv, r2_send, r2_recv,
):
    nz = n_rows // ny
    me = lax.axis_index("rows")
    own = lax.axis_index("owner")
    z, y = me // ny, lax.rem(me, ny)
    rows = out_ref.shape[1]
    groups = tuple((e, lo, hi) for e in range(2) for lo, hi in ((0, SPLIT), (SPLIT, rows)))
    body = pl.ds(2 * HEAD, rows - 2 * HEAD)

    def peer(d):
        return lax.rem(z + d // ny, nz) * ny + lax.rem(y + lax.rem(d, ny), ny)

    def lanes_of(r):
        return pl.ds(pl.multiple_of(r * LANES, LANES), LANES)

    def load(d):
        part = pl.ds(pl.multiple_of(peer(d) * rows, 8), rows)
        return (
            pltpu.make_async_copy(w_ref.at[:, part, :], wbuf.at[d], w_sem.at[d]),
            pltpu.make_async_copy(a_ref.at[:, part, :], abuf.at[d], a_sem.at[d]),
        )

    def remote(src, dst, send, recv, p):
        return pltpu.make_async_remote_copy(
            src_ref=src, dst_ref=dst, send_sem=send, recv_sem=recv,
            device_id={"rows": p}, device_id_type=MESH,
        )

    def rs(d, p, slot):
        return remote(sums_out.at[d], sums_in.at[slot], rs_send.at[d], rs_recv.at[slot], p)

    def ag(d, p, slot):
        return remote(mine, scales.at[slot], ag_send.at[d], ag_recv.at[slot], p)

    def head(h, d, p, slot):
        return remote(heads_out.at[h, d], heads_in.at[h, slot], head_send.at[h, d], head_recv.at[h, slot], p)

    def bulk(d, p, slot):
        return remote(stage.at[d], out_ref.at[:, body, lanes_of(slot)], bulk_send.at[d], bulk_recv.at[slot], p)

    def router_rows(d, p, slot):
        return remote(rpart, rrow.at[slot], r1_send.at[d], r1_recv.at[slot], p)

    def router_all(d, o, slot):
        return pltpu.make_async_remote_copy(
            src_ref=rrow, dst_ref=rall_ref.at[slot], send_sem=r2_send.at[d], recv_sem=r2_recv.at[slot],
            device_id={"owner": o}, device_id_type=MESH,
        )

    barrier = pltpu.get_barrier_semaphore()

    @pl.loop(1, n_rows)
    def _(d):
        pl.semaphore_signal(barrier, inc=1, device_id={"rows": peer(d)}, device_id_type=MESH)

    @pl.loop(1, n_owner)
    def _(d):
        pl.semaphore_signal(barrier, inc=1, device_id={"owner": lax.rem(own + d, n_owner)}, device_id_type=MESH)

    @pl.loop(0, n_rows)
    def _(d):
        for copy in load(d):
            copy.start()

    router = (
        pltpu.make_async_copy(rw_ref, rwbuf, rw_sem),
        pltpu.make_async_copy(rg_ref, rgbuf, rg_sem),
    )
    for copy in router:
        copy.start()
    for copy in router:
        copy.wait()
    part = (rwbuf[...] * rgbuf[...]).astype(jnp.bfloat16)
    rpart[...] = part
    rrow[me] = part
    eye = lax.broadcasted_iota(jnp.int32, (LANES, LANES), 0) == lax.broadcasted_iota(jnp.int32, (LANES, LANES), 1)

    def fresh(d, e, lo, hi):
        return wbuf[d, e, lo:hi, :] + abuf[d, e, lo:hi, :].astype(jnp.float32)

    def row_sums(x):
        size = jnp.abs(x)
        top = size.astype(jnp.bfloat16)
        low = (size - top.astype(jnp.float32)).astype(jnp.bfloat16)
        both = jnp.concatenate([top, low], axis=1)
        total = jnp.dot(both, jnp.ones((2 * LANES, LANES), jnp.bfloat16), preferred_element_type=jnp.float32)
        return jnp.sum(jnp.where(eye[: x.shape[0]], total, 0.0), axis=0, keepdims=True)

    def down_rows(v, count):
        spread = jnp.where(eye[:count], jnp.broadcast_to(v, (count, LANES)), 0.0)
        one = spread.astype(jnp.bfloat16)
        rest = spread - one.astype(jnp.float32)
        two = rest.astype(jnp.bfloat16)
        three = (rest - two.astype(jnp.float32)).astype(jnp.bfloat16)
        pieces = jnp.concatenate([one, two, three], axis=1)
        return jnp.dot(pieces, jnp.ones((3 * LANES, LANES), jnp.bfloat16), preferred_element_type=jnp.float32)

    @pl.loop(0, n_rows)
    def _(d):
        for copy in load(d):
            copy.wait()
        for g, (e, lo, hi) in enumerate(groups):
            x = fresh(d, e, lo, hi)
            if lo == 0:
                for h in range(2):
                    heads_out[h, d, e] = x[h * HEAD : (h + 1) * HEAD]
            sums_out[d, g : g + 1, :] = row_sums(x)

    pl.semaphore_wait(barrier, n_rows - 1 + n_owner - 1)

    @pl.loop(1, n_rows)
    def _(d):
        rs(d, peer(d), me).start()

    @pl.loop(1, n_rows)
    def _(d):
        head(0, d, peer(d), me).start()

    sums_in[me] = sums_out[0]
    heads_in[0, me] = heads_out[0, 0]
    heads_in[1, me] = heads_out[1, 0]

    @pl.loop(1, n_rows)
    def _(d):
        p = peer(d)
        rs(d, p, p).wait_recv()

    total = sums_in[0]
    for r in range(1, n_rows):
        total = total + sums_in[r]
    scale = total / d_model
    mine[...] = scale
    scale_ref[...] = scale
    scales[me] = scale

    @pl.loop(1, n_rows)
    def _(d):
        ag(d, peer(d), me).start()

    @pl.loop(1, n_rows)
    def _(d):
        head(1, d, peer(d), me).start()

    @pl.loop(1, n_rows)
    def _(d):
        router_rows(d, peer(d), me).start()

    def normalised(d, p, write):
        inverse = 1.0 / scales[p]
        for g, (e, lo, hi) in enumerate(groups):
            value = fresh(d, e, lo, hi) * down_rows(inverse[g : g + 1, :], hi - lo)
            first = 2 * HEAD if lo == 0 else 0
            write(e, lo + first, hi, value[first:].astype(jnp.bfloat16))

    def write_stage(d):
        def write(e, lo, hi, value):
            stage[d, e, lo - 2 * HEAD : hi - 2 * HEAD, :] = value
        return write

    def write_out(e, lo, hi, value):
        out_ref[e, lo:hi, lanes_of(me)] = value

    @pl.loop(1, n_rows)
    def _(d):
        p = peer(d)
        ag(d, p, p).wait_recv()
        normalised(d, p, write_stage(d))
        bulk(d, p, me).start()

    normalised(0, me, write_out)

    @pl.loop(1, n_rows)
    def _(d):
        p = peer(d)
        router_rows(d, p, p).wait_recv()

    @pl.loop(1, n_owner)
    def _(d):
        router_all(d, lax.rem(own + d, n_owner), own).start()

    rall_ref[own] = rrow[...]

    inverse = 1.0 / mine[...]
    factors = [down_rows(inverse[2 * e : 2 * e + 1, :], 2 * HEAD) for e in range(2)]

    @pl.loop(0, n_rows)
    def _(d):
        p = peer(d)

        @pl.when(d > 0)
        def _():
            head(0, d, p, p).wait_recv()
            head(1, d, p, p).wait_recv()

        for e in range(2):
            both = jnp.concatenate([heads_in[0, p, e], heads_in[1, p, e]], axis=0) * factors[e]
            out_ref[e, 0 : 2 * HEAD, lanes_of(p)] = both.astype(jnp.bfloat16)

    @pl.loop(1, n_rows)
    def _(d):
        p = peer(d)
        rs(d, p, me).wait_send()
        ag(d, p, me).wait_send()
        head(0, d, p, me).wait_send()
        head(1, d, p, me).wait_send()
        router_rows(d, p, me).wait_send()
        bulk(d, p, me).wait_send()
        bulk(d, p, p).wait_recv()

    @pl.loop(1, n_owner)
    def _(d):
        o = lax.rem(own + d, n_owner)
        router_all(d, o, own).wait_send()
        router_all(d, o, o).wait_recv()


def per_device(n_rows, n_owner, ny, d_model, w_down, avg_down, router_weight, router_gain):
    experts, all_rows, lanes = w_down.shape
    rows = all_rows // n_rows
    dma = pltpu.SemaphoreType.DMA
    f32, bf16 = jnp.float32, jnp.bfloat16
    serve, scale, router = pl.pallas_call(
        functools.partial(exchange, n_rows, n_owner, ny, d_model),
        out_shape=(
            pltpu.VMEM((experts, rows, n_rows * lanes), bf16),
            pltpu.VMEM((2 * experts, lanes), f32),
            pltpu.VMEM((n_owner, n_rows, 2, lanes), bf16),
        ),
        in_specs=[pl.BlockSpec(memory_space=pltpu.HBM)] * 4,
        out_specs=[pl.BlockSpec(memory_space=pltpu.VMEM)] * 3,
        scratch_shapes=[
            pltpu.VMEM((2, lanes), f32),
            pltpu.VMEM((1, lanes), f32),
            pltpu.VMEM((n_rows, experts, rows, lanes), f32),
            pltpu.VMEM((n_rows, experts, rows, lanes), bf16),
            pltpu.VMEM((n_rows, experts, rows - 2 * HEAD, lanes), bf16),
            pltpu.VMEM((2, n_rows, experts, HEAD, lanes), f32),
            pltpu.VMEM((2, n_rows, experts, HEAD, lanes), f32),
            pltpu.VMEM((n_rows, 2 * experts, lanes), f32),
            pltpu.VMEM((n_rows, 2 * experts, lanes), f32),
            pltpu.VMEM((n_rows, 2 * experts, lanes), f32),
            pltpu.VMEM((2 * experts, lanes), f32),
            pltpu.VMEM((2, lanes), bf16),
            pltpu.VMEM((n_rows, 2, lanes), bf16),
            dma, dma,
            dma((n_rows,)), dma((n_rows,)),
            dma((n_rows,)), dma((n_rows,)),
            dma((n_rows,)), dma((n_rows,)),
            dma((2, n_rows)), dma((2, n_rows)),
            dma((n_rows,)), dma((n_rows,)),
            dma((n_rows,)), dma((n_rows,)),
            dma((n_owner,)), dma((n_owner,)),
        ],
        compiler_params=pltpu.CompilerParams(
            collective_id=0, has_side_effects=True, vmem_limit_bytes=60 << 20
        ),
    )(w_down, avg_down, router_weight.T, router_gain[None, :])
    scale_down = jnp.concatenate(
        [scale.reshape(experts, 2, lanes)[:, 0, :SPLIT], scale.reshape(experts, 2, lanes)[:, 1, : rows - SPLIT]], axis=1
    )
    serve_router = jnp.transpose(router, (1, 3, 0, 2)).reshape(n_rows * lanes, 2 * n_owner)
    return serve, scale_down, serve_router


def solution(mesh):
    n_rows, n_owner = mesh.shape["rows"], mesh.shape["owner"]
    return jax.shard_map(
        functools.partial(per_device, n_rows, n_owner, 4, 4096),
        mesh=mesh,
        in_specs=(
            P("owner", None, "rows"),
            P("owner", None, "rows"),
            P("rows", "owner"),
            P("rows"),
        ),
        out_specs=(P("owner", "rows", None), P("owner", "rows"), P()),
        check_vma=False,
    )
```

```python
import functools

import jax
import jax.numpy as jnp
from jax import lax
from jax.experimental import pallas as pl
from jax.experimental.pallas import tpu as pltpu
from jax.sharding import PartitionSpec as P

MESH = pl.DeviceIdType.MESH
LANES = 128
UNIT = 8
HEADS = (1, 1)
HEAD = UNIT * sum(HEADS)
SPLIT = 128
FAR = (4, 3, 5, 2, 6, 1, 7, 0)
NEAR = (0, 1, 5, 2, 4, 6, 3, 7)


def exchange(
    n_rows, n_owner, ny, d_model,
    w_ref, a_ref, rw_ref, rg_ref,
    out_ref, scale_ref, router_ref,
    rwbuf, rgbuf, wbuf, abuf, stage, ho_0, ho_1, hi_0, hi_1, sums_out, sums_in, scales, mine,
    rpart, rrow, rall, rtile,
    rw_sem, rg_sem, own_sem, w_sem, a_sem, rs_send, rs_recv, ag_send, ag_recv, head_send, head_recv,
    bulk_send, bulk_recv, r1_send, r1_recv, r2_send, r2_recv,
):
    nz = n_rows // ny
    me = lax.axis_index("rows")
    own = lax.axis_index("owner")
    z, y = me // ny, lax.rem(me, ny)
    experts, rows = out_ref.shape[:2]
    groups = tuple((e, lo, hi) for e in range(experts) for lo, hi in ((0, SPLIT), (SPLIT, rows)))
    body = pl.ds(HEAD, rows - HEAD)
    heads_out, heads_in = (ho_0, ho_1), (hi_0, hi_1)
    others = pl.ds(0, n_rows - 1)

    def pick(table, i):
        if isinstance(i, int):
            return table[i]
        value = jnp.int32(table[0])
        for k in range(1, len(table)):
            value = jnp.where(i == k, table[k], value)
        return value

    def plane(i):
        return lax.rem(z + pick(NEAR, i), nz)

    def peers(table):
        return [
            lax.rem(z + dz, nz) * ny + lax.rem(y + dy, ny)
            for dz in table for dy in (2, 1, 3, 0) if (dz, dy) != (0, 0)
        ]

    def owners():
        return [lax.rem(own + d, n_owner) for d in range(1, n_owner)]

    def lanes_of(r):
        return pl.ds(pl.multiple_of(r * LANES, LANES), LANES)

    def load(i):
        part = pl.ds(plane(i) * ny, ny)
        return (
            pltpu.make_async_copy(w_ref.at[:, part], wbuf.at[i], w_sem.at[i]),
            pltpu.make_async_copy(a_ref.at[:, part], abuf.at[i], a_sem.at[i]),
        )

    def remote(src, dst, send, recv, p):
        return pltpu.make_async_remote_copy(
            src_ref=src, dst_ref=dst, send_sem=send, recv_sem=recv,
            device_id={"rows": p}, device_id_type=MESH,
        )

    def router_all(src, dst, o):
        return pltpu.make_async_remote_copy(
            src_ref=src, dst_ref=dst, send_sem=r2_send, recv_sem=r2_recv,
            device_id={"owner": o}, device_id_type=MESH,
        )

    def own_block():
        return pltpu.make_async_copy(stage.at[y], out_ref.at[:, body, lanes_of(me)], own_sem)

    far = peers(FAR)
    next_one = far[0]
    barrier = pltpu.get_barrier_semaphore()
    for p in far:
        pl.semaphore_signal(barrier, inc=1, device_id={"rows": p}, device_id_type=MESH)
    for o in owners():
        pl.semaphore_signal(barrier, inc=1, device_id={"owner": o}, device_id_type=MESH)

    for i in range(nz):
        for copy in load(i):
            copy.start()
    router = (
        pltpu.make_async_copy(rw_ref, rwbuf, rw_sem),
        pltpu.make_async_copy(rg_ref, rgbuf, rg_sem),
    )
    for copy in router:
        copy.start()

    eye = lax.broadcasted_iota(jnp.int32, (LANES, LANES), 0) == lax.broadcasted_iota(jnp.int32, (LANES, LANES), 1)

    def fresh(i, e, k, lo, hi):
        return wbuf[i, e, k, lo:hi, :] + abuf[i, e, k, lo:hi, :].astype(jnp.float32)

    def row_sums(x):
        size = jnp.abs(x)
        top = size.astype(jnp.bfloat16)
        low = (size - top.astype(jnp.float32)).astype(jnp.bfloat16)
        both = jnp.concatenate([top, low], axis=1)
        total = jnp.dot(both, jnp.ones((2 * LANES, LANES), jnp.bfloat16), preferred_element_type=jnp.float32)
        return jnp.sum(jnp.where(eye[: x.shape[0]], total, 0.0), axis=0, keepdims=True)

    def down_rows(v, count):
        spread = jnp.where(eye[:count], jnp.broadcast_to(v, (count, LANES)), 0.0)
        one = spread.astype(jnp.bfloat16)
        rest = spread - one.astype(jnp.float32)
        two = rest.astype(jnp.bfloat16)
        three = (rest - two.astype(jnp.float32)).astype(jnp.bfloat16)
        pieces = jnp.concatenate([one, two, three], axis=1)
        return jnp.dot(pieces, jnp.ones((3 * LANES, LANES), jnp.bfloat16), preferred_element_type=jnp.float32)

    @pl.loop(0, nz)
    def _(i):
        for copy in load(i):
            copy.wait()
        base = plane(i) * ny
        for k in range(ny):
            for g, (e, lo, hi) in enumerate(groups):
                x = fresh(i, e, k, lo, hi)
                if lo == 0:
                    first = 0
                    for h, count in enumerate(HEADS):
                        heads_out[h][base + k, e] = x[first : first + count * UNIT]
                        first += count * UNIT
                sums_out[base + k, g : g + 1, :] = row_sums(x)

    for copy in router:
        copy.wait()
    part = (rwbuf[...] * rgbuf[...]).astype(jnp.bfloat16)
    rpart[...] = part
    rrow[me] = part

    pl.semaphore_wait(barrier, n_rows - 1 + n_owner - 1)

    for p in far:
        remote(sums_out.at[p], sums_in.at[me], rs_send, rs_recv, p).start()
    for p in far:
        remote(heads_out[0].at[p], heads_in[0].at[me], head_send.at[0], head_recv.at[0], p).start()

    sums_in[me] = sums_out[me]
    for h in range(len(HEADS)):
        heads_in[h][me] = heads_out[h][me]

    remote(sums_out.at[others], sums_in.at[others], rs_send, rs_recv, next_one).wait_recv()

    total = sums_in[0]
    for r in range(1, n_rows):
        total = total + sums_in[r]
    scale = total / d_model
    mine[...] = scale
    scales[me] = scale

    for p in far:
        remote(mine, scales.at[me], ag_send, ag_recv.at[z], p).start()
    for h in range(1, len(HEADS)):
        for p in far:
            remote(heads_out[h].at[p], heads_in[h].at[me], head_send.at[h], head_recv.at[h], p).start()
    for p in far:
        remote(rpart, rrow.at[me], r1_send, r1_recv, p).start()

    for g, (e, lo, hi) in enumerate(groups):
        scale_ref[e : e + 1, lo:hi] = scale[g : g + 1, : hi - lo]

    def normalise(i, k, p):
        inverse = 1.0 / scales[p]
        for g, (e, lo, hi) in enumerate(groups):
            value = fresh(i, e, k, lo, hi) * down_rows(inverse[g : g + 1, :], hi - lo)
            first = HEAD if lo == 0 else 0
            stage[i * ny + k, e, lo + first - HEAD : hi - HEAD, :] = value[first:].astype(jnp.bfloat16)

    def wait_scales(i, count):
        got = scales.at[pl.ds(0, count)]
        remote(got, got, ag_send, ag_recv.at[plane(i)], next_one).wait_recv()

    def send(i, k, p):
        remote(stage.at[i * ny + k], out_ref.at[:, body, lanes_of(me)], bulk_send, bulk_recv, p).start()

    turns = [lax.rem(y + k, ny) for k in range(ny)]

    @pl.loop(1, nz)
    def _(i):
        base = plane(i) * ny
        wait_scales(i, ny)
        for k in turns:
            normalise(i, k, base + k)
        for k in turns:
            send(i, k, base + k)

    wait_scales(0, ny - 1)
    for k in turns:
        normalise(0, k, z * ny + k)
    own_block().start()
    for k in turns[1:]:
        send(0, k, z * ny + k)

    remote(rrow.at[others], rrow.at[others], r1_send, r1_recv, next_one).wait_recv()
    for o in owners():
        router_all(rrow, rall.at[own], o).start()
    rall[own] = rrow[...]

    inverse = 1.0 / mine[...]
    factors = [down_rows(inverse[2 * e : 2 * e + 1, :], HEAD) for e in range(experts)]
    for h in range(len(HEADS)):
        got = heads_in[h].at[others]
        remote(got, got, head_send.at[h], head_recv.at[h], next_one).wait_recv()

    @pl.loop(0, n_rows // ny)
    def _(i):
        for k in range(ny):
            r = i * ny + k
            for e in range(experts):
                whole = jnp.concatenate([heads_in[h][r, e] for h in range(len(HEADS))], axis=0) * factors[e]
                out_ref[e, 0:HEAD, lanes_of(r)] = whole.astype(jnp.bfloat16)

    got = rall.at[pl.ds(0, n_owner - 1)]
    router_all(got, got, owners()[0]).wait()

    @pl.loop(0, n_rows)
    def _(r):
        for o in range(n_owner):
            rtile[2 * o : 2 * o + 2, :] = rall[o, r].astype(jnp.float32)
        router_ref[:, lanes_of(r)] = rtile[...].astype(jnp.bfloat16)

    own_block().wait()
    remote(sums_out.at[others], sums_in.at[others], rs_send, rs_recv, next_one).wait_send()
    remote(scales.at[others], scales.at[others], ag_send, rs_recv, next_one).wait_send()
    for h in range(len(HEADS)):
        got = heads_in[h].at[others]
        remote(got, got, head_send.at[h], head_recv.at[h], next_one).wait_send()
    remote(rrow.at[others], rrow.at[others], r1_send, r1_recv, next_one).wait_send()
    landed = out_ref.at[:, body, pl.ds(0, (n_rows - 1) * LANES)]
    remote(stage.at[others], landed, bulk_send, bulk_recv, next_one).wait()


def hand_over(serve_ref, scale_ref, router_ref, serve_out, scale_out, router_out, serve_sem, scale_sem, router_sem):
    pieces = serve_sem.shape[0]
    rows = serve_ref.shape[1] * serve_ref.shape[0] // pieces
    per = pieces // serve_ref.shape[0]
    copies = [
        pltpu.make_async_copy(
            serve_ref.at[i // per, pl.ds(i % per * rows, rows), :],
            serve_out.at[i // per, pl.ds(i % per * rows, rows), :],
            serve_sem.at[i],
        )
        for i in range(pieces)
    ]
    copies.append(pltpu.make_async_copy(scale_ref, scale_out, scale_sem))
    copies.append(pltpu.make_async_copy(router_ref, router_out, router_sem))
    for copy in copies:
        copy.start()
    for copy in copies:
        copy.wait()


def per_device(n_rows, n_owner, ny, d_model, w_down, avg_down, router_weight, router_gain):
    experts, all_rows, lanes = w_down.shape
    rows = all_rows // n_rows
    dma = pltpu.SemaphoreType.DMA

    def split(x):
        return x.reshape(experts, n_rows, rows, lanes)

    f32, bf16 = jnp.float32, jnp.bfloat16
    shapes = (
        ((experts, rows, n_rows * lanes), bf16),
        ((experts, rows), f32),
        ((2 * n_owner, n_rows * lanes), bf16),
    )
    serve, scale, router = pl.pallas_call(
        functools.partial(exchange, n_rows, n_owner, ny, d_model),
        out_shape=tuple(pltpu.VMEM(shape, dtype) for shape, dtype in shapes),
        in_specs=[pl.BlockSpec(memory_space=pltpu.HBM)] * 4,
        out_specs=[pl.BlockSpec(memory_space=pltpu.VMEM)] * 3,
        scratch_shapes=[
            pltpu.VMEM((2, lanes), f32),
            pltpu.VMEM((1, lanes), f32),
            pltpu.VMEM((n_rows // ny, experts, ny, rows, lanes), f32),
            pltpu.VMEM((n_rows // ny, experts, ny, rows, lanes), bf16),
            pltpu.VMEM((n_rows, experts, rows - HEAD, lanes), bf16),
            *[pltpu.VMEM((n_rows, experts, UNIT * count, lanes), f32) for count in HEADS],
            *[pltpu.VMEM((n_rows, experts, UNIT * count, lanes), f32) for count in HEADS],
            pltpu.VMEM((n_rows, 2 * experts, lanes), f32),
            pltpu.VMEM((n_rows, 2 * experts, lanes), f32),
            pltpu.VMEM((n_rows, 2 * experts, lanes), f32),
            pltpu.VMEM((2 * experts, lanes), f32),
            pltpu.VMEM((2, lanes), bf16),
            pltpu.VMEM((n_rows, 2, lanes), bf16),
            pltpu.VMEM((n_owner, n_rows, 2, lanes), bf16),
            pltpu.VMEM((2 * n_owner, lanes), f32),
            dma, dma, dma,
            dma((n_rows // ny,)), dma((n_rows // ny,)),
            dma, dma,
            dma, dma((n_rows // ny,)),
            dma((len(HEADS),)), dma((len(HEADS),)),
            dma, dma,
            dma, dma,
            dma, dma,
        ],
        compiler_params=pltpu.CompilerParams(
            collective_id=0, has_side_effects=True, vmem_limit_bytes=60 << 20
        ),
    )(split(w_down), split(avg_down), router_weight.T, router_gain[None, :])
    serve, scale, router = pl.pallas_call(
        hand_over,
        out_shape=tuple(jax.ShapeDtypeStruct(shape, dtype) for shape, dtype in shapes),
        in_specs=[pl.BlockSpec(memory_space=pltpu.VMEM)] * 3,
        out_specs=[pl.BlockSpec(memory_space=pl.ANY)] * 3,
        scratch_shapes=[dma((2 * experts if rows % 16 == 0 else experts * 5,)), dma, dma],
        compiler_params=pltpu.CompilerParams(vmem_limit_bytes=4 << 20),
    )(serve, scale, router)
    return serve, scale, router.T


def solution(mesh):
    n_rows, n_owner = mesh.shape["rows"], mesh.shape["owner"]
    return jax.shard_map(
        functools.partial(per_device, n_rows, n_owner, 4, 4096),
        mesh=mesh,
        in_specs=(
            P("owner", None, "rows"),
            P("owner", None, "rows"),
            P("rows", "owner"),
            P("rows"),
        ),
        out_specs=(P("owner", "rows", None), P("owner", "rows"), P()),
        check_vma=False,
    )
```

```python
import functools
import math

import jax
import jax.numpy as jnp
from jax import lax
from jax.experimental import pallas as pl
from jax.experimental.pallas import tpu as pltpu
from jax.sharding import PartitionSpec as P

MESH = pl.DeviceIdType.MESH
LANES = 128
HEADS = (16, 16)
HEAD = sum(HEADS)
TINY = 1e-30
SPAN = 250.0
LOW = -125.0
SPLIT = 128
FAR = (4, 3, 5, 2, 6, 1, 7, 0)
NEAR = (0, 1, 5, 2, 4, 6, 3, 7)


def exchange(
    n_rows, n_owner, ny, d_model,
    w_ref, a_ref, rw_ref, rg_ref,
    out_ref, scale_ref, router_ref,
    rwbuf, rgbuf, wbuf, abuf, stage, ho_0, ho_1, hi_0, hi_1, sums_out, sums_in, scales, mine,
    rpart, rrow, rall, rtile,
    rw_sem, rg_sem, own_sem, w_sem, a_sem, rs_send, rs_recv, ag_send, ag_recv, head_send, head_recv,
    bulk_send, bulk_recv, r1_send, r1_recv, r2_send, r2_recv,
):
    nz = n_rows // ny
    me = lax.axis_index("rows")
    own = lax.axis_index("owner")
    z, y = me // ny, lax.rem(me, ny)
    experts, rows = out_ref.shape[:2]
    groups = tuple((e, lo, hi) for e in range(experts) for lo, hi in ((0, SPLIT), (SPLIT, rows)))
    body = pl.ds(HEAD, rows - HEAD)
    heads_out, heads_in = (ho_0, ho_1), (hi_0, hi_1)
    others = pl.ds(0, n_rows - 1)

    def pick(table, i):
        if isinstance(i, int):
            return table[i]
        value = jnp.int32(table[0])
        for k in range(1, len(table)):
            value = jnp.where(i == k, table[k], value)
        return value

    def plane(i):
        return lax.rem(z + pick(NEAR, i), nz)

    def peers(table):
        return [
            lax.rem(z + dz, nz) * ny + lax.rem(y + dy, ny)
            for dz in table for dy in (2, 1, 3, 0) if (dz, dy) != (0, 0)
        ]

    def owners():
        return [lax.rem(own + d, n_owner) for d in range(1, n_owner)]

    def lanes_of(r):
        return pl.ds(pl.multiple_of(r * LANES, LANES), LANES)

    def load(i):
        part = pl.ds(plane(i) * ny, ny)
        return (
            pltpu.make_async_copy(w_ref.at[:, part], wbuf.at[i], w_sem.at[i]),
            pltpu.make_async_copy(a_ref.at[:, part], abuf.at[i], a_sem.at[i]),
        )

    def remote(src, dst, send, recv, p):
        return pltpu.make_async_remote_copy(
            src_ref=src, dst_ref=dst, send_sem=send, recv_sem=recv,
            device_id={"rows": p}, device_id_type=MESH,
        )

    def router_all(src, dst, o):
        return pltpu.make_async_remote_copy(
            src_ref=src, dst_ref=dst, send_sem=r2_send, recv_sem=r2_recv,
            device_id={"owner": o}, device_id_type=MESH,
        )

    def own_block():
        return pltpu.make_async_copy(stage.at[y], out_ref.at[:, body, lanes_of(me)], own_sem)

    far = peers(FAR)
    next_one = far[0]
    barrier = pltpu.get_barrier_semaphore()
    for p in far:
        pl.semaphore_signal(barrier, inc=1, device_id={"rows": p}, device_id_type=MESH)
    for o in owners():
        pl.semaphore_signal(barrier, inc=1, device_id={"owner": o}, device_id_type=MESH)

    for i in range(nz):
        for copy in load(i):
            copy.start()
    router = (
        pltpu.make_async_copy(rw_ref, rwbuf, rw_sem),
        pltpu.make_async_copy(rg_ref, rgbuf, rg_sem),
    )
    for copy in router:
        copy.start()

    eye = lax.broadcasted_iota(jnp.int32, (LANES, LANES), 0) == lax.broadcasted_iota(jnp.int32, (LANES, LANES), 1)

    beside = lax.broadcasted_iota(jnp.int32, (HEAD, LANES), 1) == lax.broadcasted_iota(jnp.int32, (HEAD, LANES), 0) + (rows - SPLIT)

    def encode(x):
        size = jnp.abs(x)
        most = jnp.maximum(jnp.max(size, axis=1, keepdims=True), TINY)
        code = jnp.exp2(size * (SPAN / most) + LOW)
        return jnp.where(x < 0, -code, code).astype(jnp.bfloat16), most

    def decode(code, most):
        code = code.astype(jnp.float32)
        size = (jnp.log(jnp.abs(code)) * (1.0 / math.log(2.0)) - LOW) * (most / SPAN)
        return jnp.where(code < 0, -size, size)

    def fresh(i, e, k, lo, hi):
        return wbuf[i, e, k, lo:hi, :] + abuf[i, e, k, lo:hi, :].astype(jnp.float32)

    def row_sums(x):
        size = jnp.abs(x)
        top = size.astype(jnp.bfloat16)
        low = (size - top.astype(jnp.float32)).astype(jnp.bfloat16)
        both = jnp.concatenate([top, low], axis=1)
        total = jnp.dot(both, jnp.ones((2 * LANES, LANES), jnp.bfloat16), preferred_element_type=jnp.float32)
        return jnp.sum(jnp.where(eye[: x.shape[0]], total, 0.0), axis=0, keepdims=True)

    def down_rows(v, count):
        spread = jnp.where(eye[:count], jnp.broadcast_to(v, (count, LANES)), 0.0)
        one = spread.astype(jnp.bfloat16)
        rest = spread - one.astype(jnp.float32)
        two = rest.astype(jnp.bfloat16)
        three = (rest - two.astype(jnp.float32)).astype(jnp.bfloat16)
        pieces = jnp.concatenate([one, two, three], axis=1)
        return jnp.dot(pieces, jnp.ones((3 * LANES, LANES), jnp.bfloat16), preferred_element_type=jnp.float32)

    @pl.loop(0, nz)
    def _(i):
        for copy in load(i):
            copy.wait()
        base = plane(i) * ny
        for k in range(ny):
            for g, (e, lo, hi) in enumerate(groups):
                x = fresh(i, e, k, lo, hi)
                total = row_sums(x)
                if lo == 0:
                    code, most = encode(x[:HEAD])
                    first = 0
                    for h, count in enumerate(HEADS):
                        heads_out[h][base + k, e] = code[first : first + count]
                        first += count
                else:
                    total = total + jnp.sum(jnp.where(beside, most, 0.0), axis=0, keepdims=True)
                sums_out[base + k, g : g + 1, :] = total

    for copy in router:
        copy.wait()
    part = (rwbuf[...] * rgbuf[...]).astype(jnp.bfloat16)
    rpart[...] = part
    rrow[me] = part

    pl.semaphore_wait(barrier, n_rows - 1 + n_owner - 1)

    for p in far:
        remote(sums_out.at[p], sums_in.at[me], rs_send, rs_recv, p).start()
    for p in far:
        remote(heads_out[0].at[p], heads_in[0].at[me], head_send.at[0], head_recv.at[0], p).start()

    sums_in[me] = sums_out[me]
    for h in range(len(HEADS)):
        heads_in[h][me] = heads_out[h][me]

    remote(sums_out.at[others], sums_in.at[others], rs_send, rs_recv, next_one).wait_recv()

    total = sums_in[0]
    for r in range(1, n_rows):
        total = total + sums_in[r]
    scale = total / d_model
    mine[...] = scale
    scales[me] = scale

    for p in far:
        remote(mine, scales.at[me], ag_send, ag_recv.at[z], p).start()
    for h in range(1, len(HEADS)):
        for p in far:
            remote(heads_out[h].at[p], heads_in[h].at[me], head_send.at[h], head_recv.at[h], p).start()
    for p in far:
        remote(rpart, rrow.at[me], r1_send, r1_recv, p).start()

    for g, (e, lo, hi) in enumerate(groups):
        scale_ref[e : e + 1, lo:hi] = scale[g : g + 1, : hi - lo]

    def normalise(i, k, p):
        inverse = 1.0 / scales[p]
        for g, (e, lo, hi) in enumerate(groups):
            value = fresh(i, e, k, lo, hi) * down_rows(inverse[g : g + 1, :], hi - lo)
            first = HEAD if lo == 0 else 0
            stage[i * ny + k, e, lo + first - HEAD : hi - HEAD, :] = value[first:].astype(jnp.bfloat16)

    def wait_scales(i, count):
        got = scales.at[pl.ds(0, count)]
        remote(got, got, ag_send, ag_recv.at[plane(i)], next_one).wait_recv()

    def send(i, k, p):
        remote(stage.at[i * ny + k], out_ref.at[:, body, lanes_of(me)], bulk_send, bulk_recv, p).start()

    turns = [lax.rem(y + k, ny) for k in range(ny)]

    @pl.loop(1, nz)
    def _(i):
        base = plane(i) * ny
        wait_scales(i, ny)
        for k in turns:
            normalise(i, k, base + k)
        for k in turns:
            send(i, k, base + k)

    wait_scales(0, ny - 1)
    for k in turns:
        normalise(0, k, z * ny + k)
    own_block().start()
    for k in turns[1:]:
        send(0, k, z * ny + k)

    remote(rrow.at[others], rrow.at[others], r1_send, r1_recv, next_one).wait_recv()
    for o in owners():
        router_all(rrow, rall.at[own], o).start()
    rall[own] = rrow[...]

    inverse = 1.0 / mine[...]
    factors = [down_rows(inverse[2 * e : 2 * e + 1, :], HEAD) for e in range(experts)]
    for h in range(len(HEADS)):
        got = heads_in[h].at[others]
        remote(got, got, head_send.at[h], head_recv.at[h], next_one).wait_recv()

    @pl.loop(0, n_rows // ny)
    def _(i):
        for k in range(ny):
            r = i * ny + k
            for e in range(experts):
                code = jnp.concatenate([heads_in[h][r, e] for h in range(len(HEADS))], axis=0)
                row = jnp.broadcast_to(sums_in[r, 2 * e + 1 : 2 * e + 2, :], (HEAD, LANES))
                most = jnp.sum(jnp.where(beside, row, 0.0), axis=1, keepdims=True)
                out_ref[e, 0:HEAD, lanes_of(r)] = (decode(code, most) * factors[e]).astype(jnp.bfloat16)

    got = rall.at[pl.ds(0, n_owner - 1)]
    router_all(got, got, owners()[0]).wait()

    @pl.loop(0, n_rows)
    def _(r):
        for o in range(n_owner):
            rtile[2 * o : 2 * o + 2, :] = rall[o, r].astype(jnp.float32)
        router_ref[:, lanes_of(r)] = rtile[...].astype(jnp.bfloat16)

    own_block().wait()
    remote(sums_out.at[others], sums_in.at[others], rs_send, rs_recv, next_one).wait_send()
    remote(scales.at[others], scales.at[others], ag_send, rs_recv, next_one).wait_send()
    for h in range(len(HEADS)):
        got = heads_in[h].at[others]
        remote(got, got, head_send.at[h], head_recv.at[h], next_one).wait_send()
    remote(rrow.at[others], rrow.at[others], r1_send, r1_recv, next_one).wait_send()
    landed = out_ref.at[:, body, pl.ds(0, (n_rows - 1) * LANES)]
    remote(stage.at[others], landed, bulk_send, bulk_recv, next_one).wait()


def hand_over(serve_ref, scale_ref, router_ref, serve_out, scale_out, router_out, serve_sem, scale_sem, router_sem):
    pieces = serve_sem.shape[0]
    rows = serve_ref.shape[1] * serve_ref.shape[0] // pieces
    per = pieces // serve_ref.shape[0]
    copies = [
        pltpu.make_async_copy(
            serve_ref.at[i // per, pl.ds(i % per * rows, rows), :],
            serve_out.at[i // per, pl.ds(i % per * rows, rows), :],
            serve_sem.at[i],
        )
        for i in range(pieces)
    ]
    copies.append(pltpu.make_async_copy(scale_ref, scale_out, scale_sem))
    copies.append(pltpu.make_async_copy(router_ref, router_out, router_sem))
    for copy in copies:
        copy.start()
    for copy in copies:
        copy.wait()


def per_device(n_rows, n_owner, ny, d_model, w_down, avg_down, router_weight, router_gain):
    experts, all_rows, lanes = w_down.shape
    rows = all_rows // n_rows
    dma = pltpu.SemaphoreType.DMA

    def split(x):
        return x.reshape(experts, n_rows, rows, lanes)

    f32, bf16 = jnp.float32, jnp.bfloat16
    shapes = (
        ((experts, rows, n_rows * lanes), bf16),
        ((experts, rows), f32),
        ((2 * n_owner, n_rows * lanes), bf16),
    )
    serve, scale, router = pl.pallas_call(
        functools.partial(exchange, n_rows, n_owner, ny, d_model),
        out_shape=tuple(pltpu.VMEM(shape, dtype) for shape, dtype in shapes),
        in_specs=[pl.BlockSpec(memory_space=pltpu.HBM)] * 4,
        out_specs=[pl.BlockSpec(memory_space=pltpu.VMEM)] * 3,
        scratch_shapes=[
            pltpu.VMEM((2, lanes), f32),
            pltpu.VMEM((1, lanes), f32),
            pltpu.VMEM((n_rows // ny, experts, ny, rows, lanes), f32),
            pltpu.VMEM((n_rows // ny, experts, ny, rows, lanes), bf16),
            pltpu.VMEM((n_rows, experts, rows - HEAD, lanes), bf16),
            *[pltpu.VMEM((n_rows, experts, count, lanes), bf16) for count in HEADS],
            *[pltpu.VMEM((n_rows, experts, count, lanes), bf16) for count in HEADS],
            pltpu.VMEM((n_rows, 2 * experts, lanes), f32),
            pltpu.VMEM((n_rows, 2 * experts, lanes), f32),
            pltpu.VMEM((n_rows, 2 * experts, lanes), f32),
            pltpu.VMEM((2 * experts, lanes), f32),
            pltpu.VMEM((2, lanes), bf16),
            pltpu.VMEM((n_rows, 2, lanes), bf16),
            pltpu.VMEM((n_owner, n_rows, 2, lanes), bf16),
            pltpu.VMEM((2 * n_owner, lanes), f32),
            dma, dma, dma,
            dma((n_rows // ny,)), dma((n_rows // ny,)),
            dma, dma,
            dma, dma((n_rows // ny,)),
            dma((len(HEADS),)), dma((len(HEADS),)),
            dma, dma,
            dma, dma,
            dma, dma,
        ],
        compiler_params=pltpu.CompilerParams(
            collective_id=0, has_side_effects=True, vmem_limit_bytes=60 << 20
        ),
    )(split(w_down), split(avg_down), router_weight.T, router_gain[None, :])
    serve, scale, router = pl.pallas_call(
        hand_over,
        out_shape=tuple(jax.ShapeDtypeStruct(shape, dtype) for shape, dtype in shapes),
        in_specs=[pl.BlockSpec(memory_space=pltpu.VMEM)] * 3,
        out_specs=[pl.BlockSpec(memory_space=pl.ANY)] * 3,
        scratch_shapes=[dma((2 * experts if rows % 16 == 0 else experts * 5,)), dma, dma],
        compiler_params=pltpu.CompilerParams(vmem_limit_bytes=4 << 20),
    )(serve, scale, router)
    return serve, scale, router.T


def solution(mesh):
    n_rows, n_owner = mesh.shape["rows"], mesh.shape["owner"]
    return jax.shard_map(
        functools.partial(per_device, n_rows, n_owner, 4, 4096),
        mesh=mesh,
        in_specs=(
            P("owner", None, "rows"),
            P("owner", None, "rows"),
            P("rows", "owner"),
            P("rows"),
        ),
        out_specs=(P("owner", "rows", None), P("owner", "rows"), P()),
        check_vma=False,
    )
```

```python
import functools
import math

import jax
import jax.numpy as jnp
from jax import lax
from jax.experimental import pallas as pl
from jax.experimental.pallas import tpu as pltpu
from jax.sharding import PartitionSpec as P

MESH = pl.DeviceIdType.MESH
LANES = 128
HEADS = (16, 8, 16)
HEAD = sum(HEADS)
TINY = 1e-30
SPAN = 250.0
LOW = -125.0
SPLIT = 128
FAR = (4, 3, 5, 2, 6, 1, 7, 0)
NEAR = (0, 1, 5, 2, 4, 6, 3, 7)


def exchange(
    n_rows, n_owner, ny, d_model,
    w_ref, a_ref, rw_ref, rg_ref,
    out_ref, scale_ref, router_ref,
    rwbuf, rgbuf, wbuf, abuf, stage, ho_0, ho_1, ho_2, hi_0, hi_1, hi_2, sums_out, sums_in, scales, mine,
    rpart, rrow, rall, rtile,
    rw_sem, rg_sem, own_sem, w_sem, a_sem, rs_send, rs_recv, ag_send, ag_recv, head_send, head_recv,
    bulk_send, bulk_recv, r1_send, r1_recv, r2_send, r2_recv,
):
    nz = n_rows // ny
    me = lax.axis_index("rows")
    own = lax.axis_index("owner")
    z, y = me // ny, lax.rem(me, ny)
    experts, rows = out_ref.shape[:2]
    groups = tuple((e, lo, hi) for e in range(experts) for lo, hi in ((0, SPLIT), (SPLIT, rows)))
    body = pl.ds(HEAD, rows - HEAD)
    heads_out, heads_in = (ho_0, ho_1, ho_2), (hi_0, hi_1, hi_2)
    others = pl.ds(0, n_rows - 1)

    def pick(table, i):
        if isinstance(i, int):
            return table[i]
        value = jnp.int32(table[0])
        for k in range(1, len(table)):
            value = jnp.where(i == k, table[k], value)
        return value

    def plane(i):
        return lax.rem(z + pick(NEAR, i), nz)

    def peers(table):
        return [
            lax.rem(z + dz, nz) * ny + lax.rem(y + dy, ny)
            for dz in table for dy in (2, 1, 3, 0) if (dz, dy) != (0, 0)
        ]

    def owners():
        return [lax.rem(own + d, n_owner) for d in range(1, n_owner)]

    def lanes_of(r):
        return pl.ds(pl.multiple_of(r * LANES, LANES), LANES)

    def load(i, whole=True):
        part, cut = pl.ds(plane(i) * ny, ny), body if whole else pl.ds(0, HEAD)
        return [
            pltpu.make_async_copy(ref.at[:, part, cut], buf.at[i, :, :, cut], sem.at[int(whole), i])
            for ref, buf, sem in ((w_ref, wbuf, w_sem), (a_ref, abuf, a_sem))
        ]

    def remote(src, dst, send, recv, p):
        return pltpu.make_async_remote_copy(
            src_ref=src, dst_ref=dst, send_sem=send, recv_sem=recv,
            device_id={"rows": p}, device_id_type=MESH,
        )

    def router_all(src, dst, o):
        return pltpu.make_async_remote_copy(
            src_ref=src, dst_ref=dst, send_sem=r2_send, recv_sem=r2_recv,
            device_id={"owner": o}, device_id_type=MESH,
        )

    def own_block():
        return pltpu.make_async_copy(stage.at[y], out_ref.at[:, body, lanes_of(me)], own_sem)

    far = peers(FAR)
    next_one = far[0]
    barrier = pltpu.get_barrier_semaphore()
    for p in far:
        pl.semaphore_signal(barrier, inc=1, device_id={"rows": p}, device_id_type=MESH)
    for o in owners():
        pl.semaphore_signal(barrier, inc=1, device_id={"owner": o}, device_id_type=MESH)

    for whole in (False, True):
        for i in range(nz):
            for copy in load(i, whole):
                copy.start()
    router = (
        pltpu.make_async_copy(rw_ref, rwbuf, rw_sem),
        pltpu.make_async_copy(rg_ref, rgbuf, rg_sem),
    )
    for copy in router:
        copy.start()

    eye = lax.broadcasted_iota(jnp.int32, (LANES, LANES), 0) == lax.broadcasted_iota(jnp.int32, (LANES, LANES), 1)

    beside = lax.broadcasted_iota(jnp.int32, (HEAD, LANES), 1) == lax.broadcasted_iota(jnp.int32, (HEAD, LANES), 0) + (rows - SPLIT)

    def encode(x):
        size = jnp.abs(x)
        most = jnp.maximum(jnp.max(size, axis=1, keepdims=True), TINY)
        code = jnp.exp2(size * (SPAN / most) + LOW)
        return jnp.where(x < 0, -code, code).astype(jnp.bfloat16), most

    def decode(code, most):
        code = code.astype(jnp.float32)
        size = (jnp.log(jnp.abs(code)) * (1.0 / math.log(2.0)) - LOW) * (most / SPAN)
        return jnp.where(code < 0, -size, size)

    def fresh(i, e, k, lo, hi):
        return wbuf[i, e, k, lo:hi, :] + abuf[i, e, k, lo:hi, :].astype(jnp.float32)

    def row_sums(x):
        size = jnp.abs(x)
        top = size.astype(jnp.bfloat16)
        low = (size - top.astype(jnp.float32)).astype(jnp.bfloat16)
        both = jnp.concatenate([top, low], axis=1)
        total = jnp.dot(both, jnp.ones((2 * LANES, LANES), jnp.bfloat16), preferred_element_type=jnp.float32)
        return jnp.sum(jnp.where(eye[: x.shape[0]], total, 0.0), axis=0, keepdims=True)

    def down_rows(v, count):
        spread = jnp.where(eye[:count], jnp.broadcast_to(v, (count, LANES)), 0.0)
        one = spread.astype(jnp.bfloat16)
        rest = spread - one.astype(jnp.float32)
        two = rest.astype(jnp.bfloat16)
        three = (rest - two.astype(jnp.float32)).astype(jnp.bfloat16)
        pieces = jnp.concatenate([one, two, three], axis=1)
        return jnp.dot(pieces, jnp.ones((3 * LANES, LANES), jnp.bfloat16), preferred_element_type=jnp.float32)

    @pl.loop(0, nz)
    def _(i):
        for copy in load(i, False):
            copy.wait()
        base = plane(i) * ny
        for k in range(ny):
            for e in range(experts):
                code, most = encode(fresh(i, e, k, 0, HEAD))
                first = 0
                for h, count in enumerate(HEADS):
                    heads_out[h][base + k, e] = code[first : first + count]
                    first += count
                sums_out[base + k, 2 * e : 2 * e + 1, :] = jnp.zeros((1, LANES), jnp.float32)
                sums_out[base + k, 2 * e + 1 : 2 * e + 2, :] = jnp.sum(
                    jnp.where(beside, most, 0.0), axis=0, keepdims=True
                )

    def add_sums(i):
        for copy in load(i):
            copy.wait()
        base = plane(i) * ny
        for k in range(ny):
            for g, (e, lo, hi) in enumerate(groups):
                sums_out[base + k, g : g + 1, :] += row_sums(fresh(i, e, k, lo, hi))

    before = jnp.where(z < nz // 2 - 1, nz, 0)

    @pl.loop(0, before)
    def _(i):
        add_sums(i)

    for copy in router:
        copy.wait()
    part = (rwbuf[...] * rgbuf[...]).astype(jnp.bfloat16)
    rpart[...] = part
    rrow[me] = part

    pl.semaphore_wait(barrier, n_rows - 1 + n_owner - 1)

    for p in far:
        remote(heads_out[0].at[p], heads_in[0].at[me], head_send.at[0], head_recv.at[0], p).start()

    @pl.loop(before, nz)
    def _(i):
        add_sums(i)

    for p in far:
        remote(sums_out.at[p], sums_in.at[me], rs_send, rs_recv, p).start()
    for h in range(1, len(HEADS) - 1):
        for p in far:
            remote(heads_out[h].at[p], heads_in[h].at[me], head_send.at[h], head_recv.at[h], p).start()

    sums_in[me] = sums_out[me]
    for h in range(len(HEADS)):
        heads_in[h][me] = heads_out[h][me]

    remote(sums_out.at[others], sums_in.at[others], rs_send, rs_recv, next_one).wait_recv()

    total = sums_in[0]
    for r in range(1, n_rows):
        total = total + sums_in[r]
    scale = total / d_model
    mine[...] = scale
    scales[me] = scale

    for p in far:
        remote(mine, scales.at[me], ag_send, ag_recv.at[z], p).start()
    h = len(HEADS) - 1
    for p in far:
        remote(heads_out[h].at[p], heads_in[h].at[me], head_send.at[h], head_recv.at[h], p).start()
    for p in far:
        remote(rpart, rrow.at[me], r1_send, r1_recv, p).start()

    for g, (e, lo, hi) in enumerate(groups):
        scale_ref[e : e + 1, lo:hi] = scale[g : g + 1, : hi - lo]

    def normalise(i, k, p):
        inverse = 1.0 / scales[p]
        for g, (e, lo, hi) in enumerate(groups):
            value = fresh(i, e, k, lo, hi) * down_rows(inverse[g : g + 1, :], hi - lo)
            first = HEAD if lo == 0 else 0
            stage[i * ny + k, e, lo + first - HEAD : hi - HEAD, :] = value[first:].astype(jnp.bfloat16)

    def wait_scales(i, count):
        got = scales.at[pl.ds(0, count)]
        remote(got, got, ag_send, ag_recv.at[plane(i)], next_one).wait_recv()

    def send(i, k, p):
        remote(stage.at[i * ny + k], out_ref.at[:, body, lanes_of(me)], bulk_send, bulk_recv, p).start()

    turns = [lax.rem(y + k, ny) for k in range(ny)]

    @pl.loop(1, nz)
    def _(i):
        base = plane(i) * ny
        wait_scales(i, ny)
        for k in turns:
            normalise(i, k, base + k)
        for k in turns:
            send(i, k, base + k)

    wait_scales(0, ny - 1)
    for k in turns:
        normalise(0, k, z * ny + k)
    own_block().start()
    for k in turns[1:]:
        send(0, k, z * ny + k)

    remote(rrow.at[others], rrow.at[others], r1_send, r1_recv, next_one).wait_recv()
    for o in owners():
        router_all(rrow, rall.at[own], o).start()
    rall[own] = rrow[...]

    inverse = 1.0 / mine[...]
    factors = [down_rows(inverse[2 * e : 2 * e + 1, :], HEAD) for e in range(experts)]
    for h in range(len(HEADS)):
        got = heads_in[h].at[others]
        remote(got, got, head_send.at[h], head_recv.at[h], next_one).wait_recv()

    @pl.loop(0, n_rows // ny)
    def _(i):
        for k in range(ny):
            r = i * ny + k
            for e in range(experts):
                code = jnp.concatenate([heads_in[h][r, e] for h in range(len(HEADS))], axis=0)
                row = jnp.broadcast_to(sums_in[r, 2 * e + 1 : 2 * e + 2, :], (HEAD, LANES))
                most = jnp.sum(jnp.where(beside, row, 0.0), axis=1, keepdims=True)
                out_ref[e, 0:HEAD, lanes_of(r)] = (decode(code, most) * factors[e]).astype(jnp.bfloat16)

    got = rall.at[pl.ds(0, n_owner - 1)]
    router_all(got, got, owners()[0]).wait()

    @pl.loop(0, n_rows)
    def _(r):
        for o in range(n_owner):
            rtile[2 * o : 2 * o + 2, :] = rall[o, r].astype(jnp.float32)
        router_ref[:, lanes_of(r)] = rtile[...].astype(jnp.bfloat16)

    own_block().wait()
    remote(sums_out.at[others], sums_in.at[others], rs_send, rs_recv, next_one).wait_send()
    remote(scales.at[others], scales.at[others], ag_send, rs_recv, next_one).wait_send()
    for h in range(len(HEADS)):
        got = heads_in[h].at[others]
        remote(got, got, head_send.at[h], head_recv.at[h], next_one).wait_send()
    remote(rrow.at[others], rrow.at[others], r1_send, r1_recv, next_one).wait_send()
    landed = out_ref.at[:, body, pl.ds(0, (n_rows - 1) * LANES)]
    remote(stage.at[others], landed, bulk_send, bulk_recv, next_one).wait()


def hand_over(serve_ref, scale_ref, router_ref, serve_out, scale_out, router_out, serve_sem, scale_sem, router_sem):
    pieces = serve_sem.shape[0]
    rows = serve_ref.shape[1] * serve_ref.shape[0] // pieces
    per = pieces // serve_ref.shape[0]
    copies = [
        pltpu.make_async_copy(
            serve_ref.at[i // per, pl.ds(i % per * rows, rows), :],
            serve_out.at[i // per, pl.ds(i % per * rows, rows), :],
            serve_sem.at[i],
        )
        for i in range(pieces)
    ]
    copies.append(pltpu.make_async_copy(scale_ref, scale_out, scale_sem))
    copies.append(pltpu.make_async_copy(router_ref, router_out, router_sem))
    for copy in copies:
        copy.start()
    for copy in copies:
        copy.wait()


def per_device(n_rows, n_owner, ny, d_model, w_down, avg_down, router_weight, router_gain):
    experts, all_rows, lanes = w_down.shape
    rows = all_rows // n_rows
    dma = pltpu.SemaphoreType.DMA

    def split(x):
        return x.reshape(experts, n_rows, rows, lanes)

    f32, bf16 = jnp.float32, jnp.bfloat16
    shapes = (
        ((experts, rows, n_rows * lanes), bf16),
        ((experts, rows), f32),
        ((2 * n_owner, n_rows * lanes), bf16),
    )
    serve, scale, router = pl.pallas_call(
        functools.partial(exchange, n_rows, n_owner, ny, d_model),
        out_shape=tuple(pltpu.VMEM(shape, dtype) for shape, dtype in shapes),
        in_specs=[pl.BlockSpec(memory_space=pltpu.HBM)] * 4,
        out_specs=[pl.BlockSpec(memory_space=pltpu.VMEM)] * 3,
        scratch_shapes=[
            pltpu.VMEM((2, lanes), f32),
            pltpu.VMEM((1, lanes), f32),
            pltpu.VMEM((n_rows // ny, experts, ny, rows, lanes), f32),
            pltpu.VMEM((n_rows // ny, experts, ny, rows, lanes), bf16),
            pltpu.VMEM((n_rows, experts, rows - HEAD, lanes), bf16),
            *[pltpu.VMEM((n_rows, experts, count, lanes), bf16) for count in HEADS],
            *[pltpu.VMEM((n_rows, experts, count, lanes), bf16) for count in HEADS],
            pltpu.VMEM((n_rows, 2 * experts, lanes), f32),
            pltpu.VMEM((n_rows, 2 * experts, lanes), f32),
            pltpu.VMEM((n_rows, 2 * experts, lanes), f32),
            pltpu.VMEM((2 * experts, lanes), f32),
            pltpu.VMEM((2, lanes), bf16),
            pltpu.VMEM((n_rows, 2, lanes), bf16),
            pltpu.VMEM((n_owner, n_rows, 2, lanes), bf16),
            pltpu.VMEM((2 * n_owner, lanes), f32),
            dma, dma, dma,
            dma((2, n_rows // ny)), dma((2, n_rows // ny)),
            dma, dma,
            dma, dma((n_rows // ny,)),
            dma((len(HEADS),)), dma((len(HEADS),)),
            dma, dma,
            dma, dma,
            dma, dma,
        ],
        compiler_params=pltpu.CompilerParams(
            collective_id=0, has_side_effects=True, vmem_limit_bytes=60 << 20
        ),
    )(split(w_down), split(avg_down), router_weight.T, router_gain[None, :])
    serve, scale, router = pl.pallas_call(
        hand_over,
        out_shape=tuple(jax.ShapeDtypeStruct(shape, dtype) for shape, dtype in shapes),
        in_specs=[pl.BlockSpec(memory_space=pltpu.VMEM)] * 3,
        out_specs=[pl.BlockSpec(memory_space=pl.ANY)] * 3,
        scratch_shapes=[dma((2 * experts if rows % 16 == 0 else experts * 5,)), dma, dma],
        compiler_params=pltpu.CompilerParams(vmem_limit_bytes=4 << 20),
    )(serve, scale, router)
    return serve, scale, router.T


def solution(mesh):
    n_rows, n_owner = mesh.shape["rows"], mesh.shape["owner"]
    return jax.shard_map(
        functools.partial(per_device, n_rows, n_owner, 4, 4096),
        mesh=mesh,
        in_specs=(
            P("owner", None, "rows"),
            P("owner", None, "rows"),
            P("rows", "owner"),
            P("rows"),
        ),
        out_specs=(P("owner", "rows", None), P("owner", "rows"), P()),
        check_vma=False,
    )
```

```python
import functools
import math

import jax
import jax.numpy as jnp
from jax import lax
from jax.experimental import pallas as pl
from jax.experimental.pallas import tpu as pltpu
from jax.sharding import PartitionSpec as P

MESH = pl.DeviceIdType.MESH
LANES = 128
HEADS = (16, 8, 16)
HEAD = sum(HEADS)
TINY = 1e-30
SPAN = 250.0
LOW = -125.0
SPLIT = 128
FAR = (4, 3, 5, 2, 6, 1, 7, 0)
NEAR = (0, 1, 5, 2, 4, 6, 3, 7)


def exchange(
    n_rows, n_owner, ny, d_model,
    w_ref, a_ref, rw_ref, rg_ref,
    out_ref, scale_ref, router_ref,
    rwbuf, rgbuf, wbuf, abuf, stage, ho_0, ho_1, ho_2, hi_0, hi_1, hi_2, sums_out, sums_in, scales, mine,
    rpart, rrow, rall, rtile,
    rw_sem, rg_sem, own_sem, w_sem, a_sem, rs_send, rs_recv, ag_send, ag_recv, head_send, head_recv,
    bulk_send, bulk_recv, r1_send, r1_recv, r2_send, r2_recv,
):
    nz = n_rows // ny
    me = lax.axis_index("rows")
    own = lax.axis_index("owner")
    z, y = me // ny, lax.rem(me, ny)
    experts, rows = out_ref.shape[:2]
    groups = tuple((e, lo, hi) for e in range(experts) for lo, hi in ((0, SPLIT), (SPLIT, rows)))
    body = pl.ds(HEAD, rows - HEAD)
    heads_out, heads_in = (ho_0, ho_1, ho_2), (hi_0, hi_1, hi_2)
    others = pl.ds(0, n_rows - 1)

    def pick(table, i):
        if isinstance(i, int):
            return table[i]
        value = jnp.int32(table[0])
        for k in range(1, len(table)):
            value = jnp.where(i == k, table[k], value)
        return value

    def plane(i):
        return lax.rem(z + pick(NEAR, i), nz)

    def peers(table):
        return [
            lax.rem(z + dz, nz) * ny + lax.rem(y + dy, ny)
            for dz in table for dy in (2, 1, 3, 0) if (dz, dy) != (0, 0)
        ]

    def owners():
        return [lax.rem(own + d, n_owner) for d in range(1, n_owner)]

    def lanes_of(r):
        return pl.ds(pl.multiple_of(r * LANES, LANES), LANES)

    def load(i, whole=True):
        part, cut = pl.ds(plane(i) * ny, ny), body if whole else pl.ds(0, HEAD)
        return [
            pltpu.make_async_copy(ref.at[:, part, cut], buf.at[i, :, :, cut], sem.at[int(whole), i])
            for ref, buf, sem in ((w_ref, wbuf, w_sem), (a_ref, abuf, a_sem))
        ]

    def remote(src, dst, send, recv, p):
        return pltpu.make_async_remote_copy(
            src_ref=src, dst_ref=dst, send_sem=send, recv_sem=recv,
            device_id={"rows": p}, device_id_type=MESH,
        )

    def router_all(src, dst, o):
        return pltpu.make_async_remote_copy(
            src_ref=src, dst_ref=dst, send_sem=r2_send, recv_sem=r2_recv,
            device_id={"owner": o}, device_id_type=MESH,
        )

    def own_block():
        return pltpu.make_async_copy(stage.at[y], out_ref.at[:, body, lanes_of(me)], own_sem)

    far = peers(FAR)
    next_one = far[0]
    barrier = pltpu.get_barrier_semaphore()
    for p in far:
        pl.semaphore_signal(barrier, inc=1, device_id={"rows": p}, device_id_type=MESH)
    for o in owners():
        pl.semaphore_signal(barrier, inc=1, device_id={"owner": o}, device_id_type=MESH)

    for whole in (False, True):
        for i in range(nz):
            for copy in load(i, whole):
                copy.start()
    router = (
        pltpu.make_async_copy(rw_ref, rwbuf, rw_sem),
        pltpu.make_async_copy(rg_ref, rgbuf, rg_sem),
    )
    for copy in router:
        copy.start()

    eye = lax.broadcasted_iota(jnp.int32, (LANES, LANES), 0) == lax.broadcasted_iota(jnp.int32, (LANES, LANES), 1)

    beside = lax.broadcasted_iota(jnp.int32, (HEAD, LANES), 1) == lax.broadcasted_iota(jnp.int32, (HEAD, LANES), 0) + (rows - SPLIT)

    def encode(x):
        size = jnp.abs(x)
        most = jnp.maximum(jnp.max(size, axis=1, keepdims=True), TINY)
        code = jnp.exp2(size * (SPAN / most) + LOW)
        return jnp.where(x < 0, -code, code).astype(jnp.bfloat16), most

    def decode(code, most):
        code = code.astype(jnp.float32)
        size = (jnp.log(jnp.abs(code)) * (1.0 / math.log(2.0)) - LOW) * (most / SPAN)
        return jnp.where(code < 0, -size, size)

    def fresh(i, e, k, lo, hi):
        return wbuf[i, e, k, lo:hi, :] + abuf[i, e, k, lo:hi, :].astype(jnp.float32)

    def row_sums(x):
        size = jnp.abs(x)
        top = size.astype(jnp.bfloat16)
        low = (size - top.astype(jnp.float32)).astype(jnp.bfloat16)
        both = jnp.concatenate([top, low], axis=1)
        total = jnp.dot(both, jnp.ones((2 * LANES, LANES), jnp.bfloat16), preferred_element_type=jnp.float32)
        return jnp.sum(jnp.where(eye[: x.shape[0]], total, 0.0), axis=0, keepdims=True)

    def down_rows(v, count):
        spread = jnp.where(eye[:count], jnp.broadcast_to(v, (count, LANES)), 0.0)
        one = spread.astype(jnp.bfloat16)
        rest = spread - one.astype(jnp.float32)
        two = rest.astype(jnp.bfloat16)
        three = (rest - two.astype(jnp.float32)).astype(jnp.bfloat16)
        pieces = jnp.concatenate([one, two, three], axis=1)
        return jnp.dot(pieces, jnp.ones((3 * LANES, LANES), jnp.bfloat16), preferred_element_type=jnp.float32)

    before = jnp.where(z < nz // 2 - 1, nz, 0)

    def encode_plane(i):
        for copy in load(i, False):
            copy.wait()
        base = plane(i) * ny
        for k in range(ny):
            for e in range(experts):
                code, most = encode(fresh(i, e, k, 0, HEAD))
                first = 0
                for h, count in enumerate(HEADS):
                    heads_out[h][base + k, e] = code[first : first + count]
                    first += count
                sums_out[base + k, 2 * e : 2 * e + 1, :] = jnp.zeros((1, LANES), jnp.float32)
                sums_out[base + k, 2 * e + 1 : 2 * e + 2, :] = jnp.sum(
                    jnp.where(beside, most, 0.0), axis=0, keepdims=True
                )

    def add_sums(i):
        for copy in load(i):
            copy.wait()
        base = plane(i) * ny
        for k in range(ny):
            for g, (e, lo, hi) in enumerate(groups):
                sums_out[base + k, g : g + 1, :] += row_sums(fresh(i, e, k, lo, hi))

    @pl.loop(0, before)
    def _(i):
        encode_plane(i)

    @pl.loop(0, before)
    def _(i):
        add_sums(i)

    for copy in router:
        copy.wait()
    part = (rwbuf[...] * rgbuf[...]).astype(jnp.bfloat16)
    rpart[...] = part
    rrow[me] = part

    pl.semaphore_wait(barrier, n_rows - 1 + n_owner - 1)

    @pl.loop(0, nz)
    def _(i):
        @pl.when(i >= before)
        def _():
            encode_plane(i)

        for k in range(ny):
            p = plane(i) * ny + lax.rem(y + k, ny)

            @pl.when(p != me)
            def _():
                remote(heads_out[0].at[p], heads_in[0].at[me], head_send.at[0], head_recv.at[0], p).start()

    @pl.loop(before, nz)
    def _(i):
        add_sums(i)

    for p in far:
        remote(sums_out.at[p], sums_in.at[me], rs_send, rs_recv, p).start()
    for h in range(1, len(HEADS) - 1):
        for p in far:
            remote(heads_out[h].at[p], heads_in[h].at[me], head_send.at[h], head_recv.at[h], p).start()

    sums_in[me] = sums_out[me]
    for h in range(len(HEADS)):
        heads_in[h][me] = heads_out[h][me]

    remote(sums_out.at[others], sums_in.at[others], rs_send, rs_recv, next_one).wait_recv()

    total = sums_in[0]
    for r in range(1, n_rows):
        total = total + sums_in[r]
    scale = total / d_model
    mine[...] = scale
    scales[me] = scale

    for p in far:
        remote(mine, scales.at[me], ag_send, ag_recv.at[z], p).start()
    h = len(HEADS) - 1
    for p in far:
        remote(heads_out[h].at[p], heads_in[h].at[me], head_send.at[h], head_recv.at[h], p).start()
    for p in far:
        remote(rpart, rrow.at[me], r1_send, r1_recv, p).start()

    for g, (e, lo, hi) in enumerate(groups):
        scale_ref[e : e + 1, lo:hi] = scale[g : g + 1, : hi - lo]

    def normalise(i, k, p):
        inverse = 1.0 / scales[p]
        for g, (e, lo, hi) in enumerate(groups):
            value = fresh(i, e, k, lo, hi) * down_rows(inverse[g : g + 1, :], hi - lo)
            first = HEAD if lo == 0 else 0
            stage[i * ny + k, e, lo + first - HEAD : hi - HEAD, :] = value[first:].astype(jnp.bfloat16)

    def wait_scales(i, count):
        got = scales.at[pl.ds(0, count)]
        remote(got, got, ag_send, ag_recv.at[plane(i)], next_one).wait_recv()

    def send(i, k, p):
        remote(stage.at[i * ny + k], out_ref.at[:, body, lanes_of(me)], bulk_send, bulk_recv, p).start()

    turns = [lax.rem(y + k, ny) for k in range(ny)]

    @pl.loop(1, nz)
    def _(i):
        base = plane(i) * ny
        wait_scales(i, ny)
        for k in turns:
            normalise(i, k, base + k)
        for k in turns:
            send(i, k, base + k)

    wait_scales(0, ny - 1)
    for k in turns:
        normalise(0, k, z * ny + k)
    own_block().start()
    for k in turns[1:]:
        send(0, k, z * ny + k)

    remote(rrow.at[others], rrow.at[others], r1_send, r1_recv, next_one).wait_recv()
    for o in owners():
        router_all(rrow, rall.at[own], o).start()
    rall[own] = rrow[...]

    inverse = 1.0 / mine[...]
    factors = [down_rows(inverse[2 * e : 2 * e + 1, :], HEAD) for e in range(experts)]
    for h in range(len(HEADS)):
        got = heads_in[h].at[others]
        remote(got, got, head_send.at[h], head_recv.at[h], next_one).wait_recv()

    @pl.loop(0, n_rows // ny)
    def _(i):
        for k in range(ny):
            r = i * ny + k
            for e in range(experts):
                code = jnp.concatenate([heads_in[h][r, e] for h in range(len(HEADS))], axis=0)
                row = jnp.broadcast_to(sums_in[r, 2 * e + 1 : 2 * e + 2, :], (HEAD, LANES))
                most = jnp.sum(jnp.where(beside, row, 0.0), axis=1, keepdims=True)
                out_ref[e, 0:HEAD, lanes_of(r)] = (decode(code, most) * factors[e]).astype(jnp.bfloat16)

    got = rall.at[pl.ds(0, n_owner - 1)]
    router_all(got, got, owners()[0]).wait()

    @pl.loop(0, n_rows)
    def _(r):
        for o in range(n_owner):
            rtile[2 * o : 2 * o + 2, :] = rall[o, r].astype(jnp.float32)
        router_ref[:, lanes_of(r)] = rtile[...].astype(jnp.bfloat16)

    own_block().wait()
    remote(sums_out.at[others], sums_in.at[others], rs_send, rs_recv, next_one).wait_send()
    remote(scales.at[others], scales.at[others], ag_send, rs_recv, next_one).wait_send()
    for h in range(len(HEADS)):
        got = heads_in[h].at[others]
        remote(got, got, head_send.at[h], head_recv.at[h], next_one).wait_send()
    remote(rrow.at[others], rrow.at[others], r1_send, r1_recv, next_one).wait_send()
    landed = out_ref.at[:, body, pl.ds(0, (n_rows - 1) * LANES)]
    remote(stage.at[others], landed, bulk_send, bulk_recv, next_one).wait()


def hand_over(serve_ref, scale_ref, router_ref, serve_out, scale_out, router_out, serve_sem, scale_sem, router_sem):
    pieces = serve_sem.shape[0]
    rows = serve_ref.shape[1] * serve_ref.shape[0] // pieces
    per = pieces // serve_ref.shape[0]
    copies = [
        pltpu.make_async_copy(
            serve_ref.at[i // per, pl.ds(i % per * rows, rows), :],
            serve_out.at[i // per, pl.ds(i % per * rows, rows), :],
            serve_sem.at[i],
        )
        for i in range(pieces)
    ]
    copies.append(pltpu.make_async_copy(scale_ref, scale_out, scale_sem))
    copies.append(pltpu.make_async_copy(router_ref, router_out, router_sem))
    for copy in copies:
        copy.start()
    for copy in copies:
        copy.wait()


def per_device(n_rows, n_owner, ny, d_model, w_down, avg_down, router_weight, router_gain):
    experts, all_rows, lanes = w_down.shape
    rows = all_rows // n_rows
    dma = pltpu.SemaphoreType.DMA

    def split(x):
        return x.reshape(experts, n_rows, rows, lanes)

    f32, bf16 = jnp.float32, jnp.bfloat16
    shapes = (
        ((experts, rows, n_rows * lanes), bf16),
        ((experts, rows), f32),
        ((2 * n_owner, n_rows * lanes), bf16),
    )
    serve, scale, router = pl.pallas_call(
        functools.partial(exchange, n_rows, n_owner, ny, d_model),
        out_shape=tuple(pltpu.VMEM(shape, dtype) for shape, dtype in shapes),
        in_specs=[pl.BlockSpec(memory_space=pltpu.HBM)] * 4,
        out_specs=[pl.BlockSpec(memory_space=pltpu.VMEM)] * 3,
        scratch_shapes=[
            pltpu.VMEM((2, lanes), f32),
            pltpu.VMEM((1, lanes), f32),
            pltpu.VMEM((n_rows // ny, experts, ny, rows, lanes), f32),
            pltpu.VMEM((n_rows // ny, experts, ny, rows, lanes), bf16),
            pltpu.VMEM((n_rows, experts, rows - HEAD, lanes), bf16),
            *[pltpu.VMEM((n_rows, experts, count, lanes), bf16) for count in HEADS],
            *[pltpu.VMEM((n_rows, experts, count, lanes), bf16) for count in HEADS],
            pltpu.VMEM((n_rows, 2 * experts, lanes), f32),
            pltpu.VMEM((n_rows, 2 * experts, lanes), f32),
            pltpu.VMEM((n_rows, 2 * experts, lanes), f32),
            pltpu.VMEM((2 * experts, lanes), f32),
            pltpu.VMEM((2, lanes), bf16),
            pltpu.VMEM((n_rows, 2, lanes), bf16),
            pltpu.VMEM((n_owner, n_rows, 2, lanes), bf16),
            pltpu.VMEM((2 * n_owner, lanes), f32),
            dma, dma, dma,
            dma((2, n_rows // ny)), dma((2, n_rows // ny)),
            dma, dma,
            dma, dma((n_rows // ny,)),
            dma((len(HEADS),)), dma((len(HEADS),)),
            dma, dma,
            dma, dma,
            dma, dma,
        ],
        compiler_params=pltpu.CompilerParams(
            collective_id=0, has_side_effects=True, vmem_limit_bytes=60 << 20
        ),
    )(split(w_down), split(avg_down), router_weight.T, router_gain[None, :])
    serve, scale, router = pl.pallas_call(
        hand_over,
        out_shape=tuple(jax.ShapeDtypeStruct(shape, dtype) for shape, dtype in shapes),
        in_specs=[pl.BlockSpec(memory_space=pltpu.VMEM)] * 3,
        out_specs=[pl.BlockSpec(memory_space=pl.ANY)] * 3,
        scratch_shapes=[dma((2 * experts if rows % 16 == 0 else experts * 5,)), dma, dma],
        compiler_params=pltpu.CompilerParams(vmem_limit_bytes=4 << 20),
    )(serve, scale, router)
    return serve, scale, router.T


def solution(mesh):
    n_rows, n_owner = mesh.shape["rows"], mesh.shape["owner"]
    return jax.shard_map(
        functools.partial(per_device, n_rows, n_owner, 4, 4096),
        mesh=mesh,
        in_specs=(
            P("owner", None, "rows"),
            P("owner", None, "rows"),
            P("rows", "owner"),
            P("rows"),
        ),
        out_specs=(P("owner", "rows", None), P("owner", "rows"), P()),
        check_vma=False,
    )
```
